32 devices in a mesh: dp: 16 (over z, y, x), tensor: 2 (over core).
Axes of the slice: x: 2, y: 2, z: 4, core: 2. Of those that a mesh axis runs over, the one named last changes fastest.
Arguments:
- vis_rows: bfloat16 [8, 128, 2, 3200], P(None, 'dp', None, 'tensor'), may hold values from -6 to 6
- ln_gain: float32 [2, 3200], replicated, may hold values from 0.25 to 1.75
- ln_bias: float32 [2, 3200], replicated, may hold values from -3 to 3
- proj_weight: bfloat16 [3200, 2, 8192], P('dp', None, 'tensor'), may hold values from -0.078125 to 0.078125
- text_rows: bfloat16 [16, 384, 8192], P('dp', None, 'tensor'), may hold values from -8 to 8
- attn_gain: float32 [8192], replicated, may hold values from 0.25 to 1.75
- w_query: bfloat16 [8192, 4096], P('dp', 'tensor'), may hold values from -0.088388348 to 0.088388348
- key_value_weight: bfloat16 [8192, 2, 1024], P('dp', None, 'tensor'), may hold values from -0.088388348 to 0.088388348
- tile_counts: int32 [16], replicated, may hold values from 1 to 16, 128 in all
- image_offsets: int32 [16], P('dp'), may hold values from 0 to 256
Outputs:
- attn_context: bfloat16 [16, 384, 4096], P('dp', None, 'tensor')
The draws below stay inside these ranges and needn't reach their ends.
Inputs may be any that keep to these rules, and one draw needn't show every extreme that they name: tile_counts counts all 128 tiles, and its largest entry is exactly 16.
All inputs are finite; a program needn't handle non-finite values.
Results may differ from the reference program's by a relative error of at most 0.0074.
Values may be sent and summed in bfloat16 or wider, within the bound.
A program may use at most 128 MiB of HBM per device.

```python
import math
import jax
import jax.numpy as jnp
import numpy as np
from jax import lax

DV = 3200
MERGE = 2
PW = 6400
MODEL_WIDTH = 8192
QUERY_HEADS = 32
KEY_VALUE_HEADS = 8
HEAD_WIDTH = 128
TILE_DEV = 8
TILE_TOK = 8
SEQUENCE_LENGTH = 384
SAMPLES = 16
TILES = 128
ROW_TOK = 128
MAXT_TILES = 16
N_DP = 16


def draw_w_query(key, part):
    bound_value = 8.0 * MODEL_WIDTH ** (-0.5)
    sampled_values = jnp.clip(jax.random.normal(jax.random.fold_in(key, 1), (MODEL_WIDTH, QUERY_HEADS * HEAD_WIDTH), jnp.float32), -4.0, 4.0) * MODEL_WIDTH ** (-0.5)
    return jnp.clip(sampled_values, -bound_value, bound_value).astype(jnp.bfloat16)


def draw_key_value_weight(key, part):
    bound_value = 8.0 * MODEL_WIDTH ** (-0.5)
    sampled_values = jnp.clip(jax.random.normal(jax.random.fold_in(key, 2), (MODEL_WIDTH, 2, KEY_VALUE_HEADS * HEAD_WIDTH), jnp.float32), -4.0, 4.0) * MODEL_WIDTH ** (-0.5)
    return jnp.clip(sampled_values, -bound_value, bound_value).astype(jnp.bfloat16)


def draw_text_rows(key, part):
    sampled_values = jnp.clip(jax.random.normal(jax.random.fold_in(key, 3), (SAMPLES, SEQUENCE_LENGTH, MODEL_WIDTH), jnp.float32), -5.0, 5.0)
    return jnp.clip(sampled_values, -8.0, 8.0).astype(jnp.bfloat16)


def with_ends(entries, own_key, smallest, top_value):
    index_at = [jax.random.randint(jax.random.fold_in(own_key, axis), (), 0, length) for axis, length in enumerate(entries.shape)]
    widest = entries.shape.index(max(entries.shape))
    beside = index_at[:widest] + [(index_at[widest] + 1) % entries.shape[widest]] + index_at[widest + 1:]
    return entries.at[tuple(index_at)].set(smallest).at[tuple(beside)].set(top_value)


def shard_levels(key, dims, pieces, smallest, largest):
    def one(axis_at, shards_of):
        draws = jax.random.uniform(jax.random.fold_in(jax.random.fold_in(key, 6), axis_at), (shards_of,), jnp.float32, smallest / len(pieces), largest / len(pieces))
        return jnp.repeat(jnp.exp(draws), dims[axis_at] // shards_of).reshape((-1,) + (1,) * (len(dims) - axis_at - 1))

    level = one(*pieces[0])
    for cut in pieces[1:]:
        level = level * one(*cut)
    return level


def profile(number_of, total, most, lean):
    loads = [(1 << 20) // math.isqrt(rank ** lean) + 1 for rank in range(2, number_of + 1)]
    spare, given = total - most - (number_of - 1), [1] * (number_of - 1)
    while spare > 0:
        movable = [i for i in range(number_of - 1) if given[i] < most]
        pool, left = sum([loads[i] for i in movable]), spare
        for i in movable:
            extra = min(most - given[i], max(1, left * loads[i] // pool), spare)
            given[i] = given[i] + extra
            spare = spare - extra
    return np.array([most] + given)


def uneven_parts(stream_key, number_of, total, most, slope):
    if number_of == 2:
        one = jax.random.randint(stream_key, (), max(1, total - most), min(most, total - 1) + 1)
        return jnp.stack([one, total - one])
    lengths = jnp.asarray(profile(number_of, total, most, slope), jnp.int32)
    couples = (number_of - 1) // 2
    source_of, receiver = lengths[1:1 + 2 * couples:2], lengths[2:2 + 2 * couples:2]
    room = jnp.minimum(source_of - 1, most - receiver)
    moved = jax.random.randint(jax.random.fold_in(stream_key, 1), (couples,), 0, 1 << 20) % (room + 1)
    lengths = lengths.at[1:1 + 2 * couples:2].set(source_of - moved).at[2:2 + 2 * couples:2].set(receiver + moved)
    return lengths[jax.random.permutation(jax.random.fold_in(stream_key, 2), number_of)]


def normal_values(own_key, dims, scale, bound, split=(), kind=jnp.bfloat16):
    level = shard_levels(own_key, dims, split, -0.22, 0.18) if split else 1.0
    entries = jax.random.normal(own_key, dims, jnp.float32) * scale * level
    return jnp.minimum(jnp.maximum(entries, -bound), bound).astype(kind)


def setup_inputs(seed: int = 0) -> dict:
    key_of = jax.random.split(jax.random.key(seed), 11)
    return {
        "vis_rows": normal_values(key_of[0], (TILE_DEV, ROW_TOK, MERGE, DV), 1.0, 6.0, ((1, 16), (3, 2))),
        "ln_gain": jnp.clip(1.0 + 0.15 * jax.random.normal(key_of[1], (MERGE, DV), jnp.float32), 0.25, 1.75),
        "ln_bias": normal_values(key_of[2], (MERGE, DV), 0.5, 3.0, (), jnp.float32),
        "proj_weight": normal_values(key_of[3], (DV, MERGE, MODEL_WIDTH), PW ** -0.5, 0.078125, ((0, 16), (2, 2))),
        "text_rows": draw_text_rows(jax.random.fold_in(key_of[10], 71), 0),
        "attn_gain": jnp.clip(1.0 + 0.15 * jax.random.normal(key_of[5], (MODEL_WIDTH,), jnp.float32), 0.25, 1.75),
        "w_query": draw_w_query(jax.random.fold_in(key_of[10], 71), 0),
        "key_value_weight": draw_key_value_weight(jax.random.fold_in(key_of[10], 71), 0),
        "tile_counts": uneven_parts(key_of[8], SAMPLES, TILES, MAXT_TILES, 2).astype(jnp.int32),
        "image_offsets": with_ends(jax.random.randint(key_of[9], (SAMPLES,), 0, SEQUENCE_LENGTH - MAXT_TILES * TILE_TOK + 1), jax.random.fold_in(key_of[9], 1), 0, SEQUENCE_LENGTH - MAXT_TILES * TILE_TOK).astype(jnp.int32),
    }


vision_epsilon = 1e-06
decoder_epsilon = 1e-05
rope_base = 500000.0

def apply_rotary(value_rows, position_indices):
    half_width = value_rows.shape[-1] // 2
    exponents = jnp.arange(half_width, dtype=jnp.float32) * (2.0 / value_rows.shape[-1])
    frequency = rope_base ** (-exponents)
    angles = position_indices.astype(jnp.float32)[:, None] * frequency[None, :]
    cosine = jnp.cos(angles)[:, None, :]
    sine = jnp.sin(angles)[:, None, :]
    first_half = value_rows[..., :half_width]
    second_half = value_rows[..., half_width:]
    return jnp.concatenate([first_half * cosine - second_half * sine, second_half * cosine + first_half * sine], axis=-1)

def layer_norm(value_rows, gain, bias_values):
    average = lax.optimization_barrier(jnp.mean(value_rows, axis=(-2, -1), keepdims=True))
    centered = value_rows - average
    variance = lax.optimization_barrier(jnp.mean(centered * centered, axis=(-2, -1), keepdims=True))
    return centered * lax.rsqrt(variance + vision_epsilon) * gain + bias_values

def decoder_sample(sequence, w_query, key_value_weight, attn_gain):
    seq_float = sequence.astype(jnp.float32)
    mean_square = lax.optimization_barrier(jnp.mean(seq_float * seq_float, axis=-1, keepdims=True))
    normalized_sequence = (seq_float * lax.rsqrt(mean_square + decoder_epsilon) * attn_gain).astype(jnp.bfloat16)
    query_full = jnp.dot(normalized_sequence, w_query, preferred_element_type=jnp.float32)
    key_value_complete = jnp.dot(normalized_sequence, key_value_weight.reshape(MODEL_WIDTH, 2 * KEY_VALUE_HEADS * HEAD_WIDTH), preferred_element_type=jnp.float32)
    key_value_complete = key_value_complete.reshape(SEQUENCE_LENGTH, 2, KEY_VALUE_HEADS * HEAD_WIDTH)
    position_indices = jnp.arange(SEQUENCE_LENGTH, dtype=jnp.int32)
    query_group_count = QUERY_HEADS // KEY_VALUE_HEADS
    query_rows = apply_rotary(query_full.reshape(SEQUENCE_LENGTH, QUERY_HEADS, HEAD_WIDTH), position_indices).astype(jnp.bfloat16)
    query_rows = query_rows.reshape(SEQUENCE_LENGTH, KEY_VALUE_HEADS, query_group_count, HEAD_WIDTH)
    key_rows = apply_rotary(key_value_complete[:, 0].reshape(SEQUENCE_LENGTH, KEY_VALUE_HEADS, HEAD_WIDTH), position_indices).astype(jnp.bfloat16)
    value_rows = key_value_complete[:, 1].reshape(SEQUENCE_LENGTH, KEY_VALUE_HEADS, HEAD_WIDTH).astype(jnp.bfloat16)
    scores = jnp.einsum('pgjd,kgd->gjpk', query_rows.astype(jnp.float32), key_rows.astype(jnp.float32)) * HEAD_WIDTH ** (-0.5)
    causal = position_indices[:, None] >= position_indices[None, :]
    scores = jnp.where(causal[None, None], scores, -1e+30)
    row_max = lax.optimization_barrier(jnp.max(scores, axis=-1, keepdims=True))
    exponentials = jnp.exp(scores - row_max)
    weights = (exponentials / lax.optimization_barrier(jnp.sum(exponentials, axis=-1, keepdims=True))).astype(jnp.bfloat16)
    context = jnp.einsum('gjpk,kgd->pgjd', weights.astype(jnp.float32), value_rows.astype(jnp.float32))
    return context.astype(jnp.bfloat16).reshape(SEQUENCE_LENGTH, QUERY_HEADS * HEAD_WIDTH)

def reference(vis_rows, ln_gain, ln_bias, proj_weight, text_rows, attn_gain, w_query, key_value_weight, tile_counts, image_offsets):
    merged = vis_rows.reshape(TILE_DEV * ROW_TOK, MERGE, DV).astype(jnp.float32)
    normed_vis = layer_norm(merged, ln_gain, ln_bias).astype(jnp.bfloat16)
    flat_weight = jnp.transpose(proj_weight, (1, 0, 2)).reshape(MERGE * DV, MODEL_WIDTH)
    image_cols = jnp.dot(normed_vis.reshape(TILE_DEV * ROW_TOK, MERGE * DV), flat_weight, preferred_element_type=jnp.float32).astype(jnp.bfloat16)
    image_tiles = image_cols.reshape(TILE_DEV, N_DP, TILE_TOK, MODEL_WIDTH).reshape(TILES, TILE_TOK, MODEL_WIDTH)
    tile_ends = jnp.cumsum(tile_counts).astype(jnp.int32)
    tile_first = (tile_ends - tile_counts).astype(jnp.int32)
    tile_order = jnp.arange(MAXT_TILES, dtype=jnp.int32)
    image_span = MAXT_TILES * TILE_TOK

    def per_sample(inputs):
        sequence, first_tile, count, offset = inputs
        picked = jnp.clip(first_tile + tile_order, 0, TILES - 1).astype(jnp.int32)
        arrived = image_tiles[picked].reshape(image_span, MODEL_WIDTH)
        start_row = offset.astype(jnp.int32)
        current = lax.dynamic_slice_in_dim(sequence, start_row, image_span, 0)
        is_image = jnp.repeat(tile_order < count, TILE_TOK)[:, None]
        merged_rows = jnp.where(is_image, arrived, current)
        sequence = lax.dynamic_update_slice_in_dim(sequence, merged_rows, start_row, 0)
        return decoder_sample(sequence, w_query, key_value_weight, attn_gain)
    return lax.map(per_sample, (text_rows, tile_first, tile_counts, image_offsets))
```

```python
import functools
import math

import jax
import jax.numpy as jnp
from jax import lax
from jax.experimental import pallas as pl
from jax.experimental.pallas import tpu as pltpu
from jax.sharding import PartitionSpec as P

QUERY_HEADS = 32
KEY_VALUE_HEADS = 8
HEAD_WIDTH = 128


vision_epsilon = 1e-06
decoder_epsilon = 1e-05
rope_base = 500000.0


def apply_rotary(value_rows, position_indices):
    half_width = value_rows.shape[-1] // 2
    exponents = jnp.arange(half_width, dtype=jnp.float32) * (2.0 / value_rows.shape[-1])
    frequency = rope_base ** (-exponents)
    angles = position_indices.astype(jnp.float32)[:, None] * frequency[None, :]
    cosine = jnp.cos(angles)[:, None, :]
    sine = jnp.sin(angles)[:, None, :]
    first_half = value_rows[..., :half_width]
    second_half = value_rows[..., half_width:]
    return jnp.concatenate(
        [first_half * cosine - second_half * sine, second_half * cosine + first_half * sine],
        axis=-1,
    )


def layer_norm(value_rows, gain, bias_values):
    average = jnp.mean(value_rows, axis=(-2, -1), keepdims=True)
    centered = value_rows - average
    variance = jnp.mean(centered * centered, axis=(-2, -1), keepdims=True)
    return centered * lax.rsqrt(variance + vision_epsilon) * gain + bias_values


MESH = pl.DeviceIdType.MESH


def partner(data_index, step, inner, plane):
    if plane is None:
        return lax.rem(data_index + step, inner)
    outer_at, inner_at = data_index // inner, data_index % inner
    if plane:
        return outer_at * inner + lax.rem(inner_at + step, inner)
    count = lax.axis_size("dp") // inner
    return lax.rem(outer_at + step, count) * inner + inner_at


def place(data_index, inner, plane):
    if plane is None:
        return data_index
    return data_index % inner if plane else data_index // inner


def greet(size, inner, plane):
    data_index = lax.axis_index("dp")
    barrier = pltpu.get_barrier_semaphore()
    for step in range(1, size):
        pl.semaphore_signal(
            barrier,
            inc=1,
            device_id={"dp": partner(data_index, step, inner, plane)},
            device_id_type=MESH,
        )
    pl.semaphore_wait(barrier, size - 1)


def exchange_kernel(size, inner, plane, x_ref, o_ref, send_sem, recv_sem, own_sem):
    data_index = lax.axis_index("dp")
    me = place(data_index, inner, plane)
    own = pltpu.make_async_copy(x_ref.at[me], o_ref.at[me], own_sem)
    own.start()
    greet(size, inner, plane)
    copies = []
    for step in range(1, size):
        target = partner(data_index, step, inner, plane)
        copy = pltpu.make_async_remote_copy(
            src_ref=x_ref.at[place(target, inner, plane)],
            dst_ref=o_ref.at[me],
            send_sem=send_sem.at[step - 1],
            recv_sem=recv_sem.at[step - 1],
            device_id={"dp": target},
            device_id_type=MESH,
        )
        copy.start()
        copies.append(copy)
    own.wait()
    for copy in copies:
        copy.wait()


def sum_kernel(size, inner, plane, rows, x_ref, o_ref, held, send_sem, recv_sem):
    data_index = lax.axis_index("dp")
    me = place(data_index, inner, plane)
    greet(size, inner, plane)
    copies = []
    for step in range(1, size):
        target = partner(data_index, step, inner, plane)
        copy = pltpu.make_async_remote_copy(
            src_ref=x_ref.at[place(target, inner, plane)],
            dst_ref=held.at[step - 1],
            send_sem=send_sem.at[step - 1],
            recv_sem=recv_sem.at[step - 1],
            device_id={"dp": target},
            device_id_type=MESH,
        )
        copy.start()
        copies.append(copy)
    for copy in copies:
        copy.wait_recv()

    def add(at, carry):
        window = pl.ds(pl.multiple_of(at * rows, rows), rows)
        total = x_ref[me, window, :].astype(jnp.float32)
        for step in range(1, size):
            total = total + held[step - 1, window, :].astype(jnp.float32)
        o_ref[window, :] = total.astype(o_ref.dtype)
        return carry

    lax.fori_loop(0, o_ref.shape[0] // rows, add, 0)
    for copy in copies:
        copy.wait_send()


def exchange(blocks, inner, plane, number):
    size = blocks.shape[0]
    return pl.pallas_call(
        functools.partial(exchange_kernel, size, inner, plane),
        out_shape=jax.ShapeDtypeStruct(blocks.shape, blocks.dtype),
        in_specs=[pl.BlockSpec(memory_space=pltpu.VMEM)],
        out_specs=pl.BlockSpec(memory_space=pltpu.VMEM),
        scratch_shapes=[
            pltpu.SemaphoreType.DMA((size - 1,)),
            pltpu.SemaphoreType.DMA((size - 1,)),
            pltpu.SemaphoreType.DMA,
        ],
        compiler_params=pltpu.CompilerParams(
            collective_id=number, has_side_effects=True, vmem_limit_bytes=40 << 20
        ),
        cost_estimate=pl.CostEstimate(
            flops=0, bytes_accessed=40 * blocks.size, transcendentals=0
        ),
    )(blocks)


def sum_blocks(blocks, inner, plane, number, kind):
    size, rows, columns = blocks.shape
    return pl.pallas_call(
        functools.partial(sum_kernel, size, inner, plane, math.gcd(rows, 16)),
        out_shape=jax.ShapeDtypeStruct((rows, columns), kind),
        in_specs=[pl.BlockSpec(memory_space=pltpu.VMEM)],
        out_specs=pl.BlockSpec(memory_space=pltpu.VMEM),
        scratch_shapes=[
            pltpu.VMEM((size - 1, rows, columns), blocks.dtype),
            pltpu.SemaphoreType.DMA((size - 1,)),
            pltpu.SemaphoreType.DMA((size - 1,)),
        ],
        compiler_params=pltpu.CompilerParams(
            collective_id=number, has_side_effects=True, vmem_limit_bytes=40 << 20
        ),
        cost_estimate=pl.CostEstimate(
            flops=0, bytes_accessed=40 * blocks.size, transcendentals=0
        ),
    )(blocks)


def tensor_pieces(block):
    count = lax.axis_size("tensor")
    pieces = [block]
    for step in range(1, count):
        ring = [(at, (at + step) % count) for at in range(count)]
        pieces.append(lax.ppermute(block, "tensor", ring))
    return pieces


def attend(query_full, key_value_complete):
    seq_len = query_full.shape[0]
    query_group_count = QUERY_HEADS // KEY_VALUE_HEADS
    local_kv = key_value_complete.shape[2] // HEAD_WIDTH
    local_query = query_full.shape[1] // HEAD_WIDTH
    position_indices = jnp.arange(seq_len, dtype=jnp.int32)
    query_rows = apply_rotary(
        query_full.reshape(seq_len, local_query, HEAD_WIDTH), position_indices
    ).astype(jnp.bfloat16)
    query_rows = query_rows.reshape(seq_len, local_kv, query_group_count, HEAD_WIDTH)
    key_rows = apply_rotary(
        key_value_complete[:, 0].reshape(seq_len, local_kv, HEAD_WIDTH), position_indices
    ).astype(jnp.bfloat16)
    value_rows = (
        key_value_complete[:, 1].reshape(seq_len, local_kv, HEAD_WIDTH).astype(jnp.bfloat16)
    )
    scores = jnp.einsum(
        "pgjd,kgd->gjpk", query_rows, key_rows, preferred_element_type=jnp.float32
    ) * HEAD_WIDTH ** (-0.5)
    causal = position_indices[:, None] >= position_indices[None, :]
    scores = jnp.where(causal[None, None], scores, -1e30)
    row_max = jnp.max(scores, axis=-1, keepdims=True)
    exponentials = jnp.exp(scores - row_max)
    weights = (exponentials / jnp.sum(exponentials, axis=-1, keepdims=True)).astype(jnp.bfloat16)
    context = jnp.einsum("gjpk,kgd->pgjd", weights, value_rows, preferred_element_type=jnp.float32)
    return context.astype(jnp.bfloat16).reshape(seq_len, local_query * HEAD_WIDTH)


def per_device(
    vis_rows,
    ln_gain,
    ln_bias,
    proj_weight,
    text_rows,
    attn_gain,
    w_query,
    key_value_weight,
    tile_counts,
    image_offsets,
):
    data_count = lax.axis_size("dp")
    data_index = lax.axis_index("dp")
    tensor_count = lax.axis_size("tensor")
    tensor_index = lax.axis_index("tensor")
    tile_rows, tile_tok, merge_count, part_width = vis_rows.shape
    vision_width = ln_gain.shape[1]
    part_model = proj_weight.shape[2]
    token_count = tile_rows * tile_tok
    inner = 1 << (int(math.log2(data_count)) // 2)
    outer = data_count // inner
    columns_of = [[at * inner + b for at in range(outer)] for b in range(inner)]
    depth = w_query.shape[0]
    weight = jnp.concatenate([w_query, key_value_weight.reshape(depth, -1)], axis=1)
    weight = lax.all_gather(weight, "dp", axis=0, tiled=True, axis_index_groups=columns_of)

    max_tiles = 2 * tile_rows
    slot_count = (max_tiles + data_count - 1) // data_count
    tile_ends = jnp.cumsum(tile_counts)
    tile_firsts = tile_ends - tile_counts
    sample_ids = jnp.arange(data_count, dtype=jnp.int32)
    tiles_here = jnp.arange(tile_rows, dtype=jnp.int32) * data_count + data_index
    owners = jnp.sum((tile_ends[None, :] <= tiles_here[:, None]).astype(jnp.int32), axis=1)
    owner_first = jnp.sum(
        jnp.where(sample_ids[None, :] == owners[:, None], tile_firsts[None, :], 0), axis=1
    )
    slots = (tiles_here - owner_first) // data_count
    is_mine = sample_ids == data_index
    my_first = jnp.sum(jnp.where(is_mine, tile_firsts, 0))
    my_count = jnp.sum(jnp.where(is_mine, tile_counts, 0))
    tile_order = jnp.arange(max_tiles, dtype=jnp.int32)
    sources = (my_first + tile_order) % data_count
    slot_index = tile_order // data_count
    image_span = max_tiles * tile_tok

    pieces = tensor_pieces(vis_rows.reshape(token_count, merge_count, part_width))
    whole = jnp.zeros((token_count, merge_count, vision_width), vis_rows.dtype)
    for step, piece in enumerate(pieces):
        start = (tensor_index - step) % tensor_count * part_width
        whole = lax.dynamic_update_slice_in_dim(whole, piece, start, 2)
    normed_vis = layer_norm(whole.astype(jnp.float32), ln_gain, ln_bias).astype(jnp.bfloat16)
    feature = vision_width // data_count
    blocks = normed_vis.reshape(token_count, merge_count, data_count, feature)
    blocks = blocks.transpose(2, 0, 1, 3).reshape(data_count, token_count, merge_count * feature)
    blocks = exchange(blocks, data_count, None, 0)
    proj = proj_weight.transpose(1, 0, 2).reshape(merge_count * feature, part_model)
    partial = jnp.dot(
        blocks.reshape(data_count * token_count, merge_count * feature),
        proj,
        preferred_element_type=jnp.float32,
    ).astype(jnp.bfloat16)
    partial = partial.reshape(outer, inner, token_count, part_model).transpose(1, 0, 2, 3)
    partial = sum_blocks(
        partial.reshape(inner, outer * token_count, part_model), inner, True, 1, jnp.bfloat16
    )
    image_cols = sum_blocks(
        partial.reshape(outer, token_count, part_model), inner, False, 2, jnp.bfloat16
    ).reshape(tile_rows, tile_tok, part_model)

    empty_slots = jnp.zeros((data_count, slot_count) + image_cols.shape[1:], jnp.bfloat16)
    routed = empty_slots.at[owners, slots].set(image_cols)
    received = exchange(routed, data_count, None, 3)
    arrived = received[sources, slot_index]
    arrived = arrived.reshape(image_span, part_model)
    start_row = image_offsets[0]
    sequence = text_rows[0]
    current = lax.dynamic_slice_in_dim(sequence, start_row, image_span, 0)
    is_image = jnp.repeat(tile_order < my_count, tile_tok)[:, None]
    combined = jnp.where(is_image, arrived, current)
    sequence = lax.dynamic_update_slice_in_dim(sequence, combined, start_row, 0)

    seq_len = sequence.shape[0]
    model_width = attn_gain.shape[0]
    seq_float = sequence.astype(jnp.float32)
    squares = lax.psum(jnp.sum(seq_float * seq_float, axis=-1), "tensor")[:, None]
    gain = lax.dynamic_slice_in_dim(attn_gain, tensor_index * part_model, part_model, 0)
    normalized = (
        seq_float * lax.rsqrt(squares / model_width + decoder_epsilon) * gain
    ).astype(jnp.bfloat16)
    held_rows = part_model // depth // inner
    normalized = normalized.reshape(seq_len, held_rows, inner, depth).transpose(2, 0, 1, 3)
    normalized = exchange(
        normalized.reshape(inner, seq_len, held_rows * depth), inner, True, 4
    ).reshape(inner * seq_len, held_rows * depth)
    product = 0.0
    for step, piece in enumerate(tensor_pieces(normalized)):
        start = (tensor_index - step) % tensor_count * (held_rows * depth)
        rows = lax.dynamic_slice_in_dim(weight, start, held_rows * depth, 0)
        product = product + jnp.dot(piece, rows, preferred_element_type=jnp.float32)
    product = product.astype(jnp.bfloat16).reshape(inner, seq_len, -1)
    product = sum_blocks(product, inner, True, 5, jnp.float32)
    part_query = w_query.shape[1]
    context = attend(product[:, :part_query], product[:, part_query:].reshape(seq_len, 2, -1))
    return context.reshape(1, seq_len, context.shape[1])


def solution(mesh):
    in_specs = (
        P(None, "dp", None, "tensor"),
        P(),
        P(),
        P("dp", None, "tensor"),
        P("dp", None, "tensor"),
        P(),
        P("dp", "tensor"),
        P("dp", None, "tensor"),
        P(),
        P("dp"),
    )
    out_specs = P("dp", None, "tensor")
    return jax.shard_map(
        per_device, mesh=mesh, in_specs=in_specs, out_specs=out_specs, check_vma=False
    )
```

```python
import functools
import math

import jax
import jax.numpy as jnp
from jax import lax
from jax.experimental import pallas as pl
from jax.experimental.pallas import tpu as pltpu
from jax.sharding import PartitionSpec as P

QUERY_HEADS = 32
KEY_VALUE_HEADS = 8
HEAD_WIDTH = 128


vision_epsilon = 1e-06
decoder_epsilon = 1e-05
rope_base = 500000.0


def layer_norm(value_rows, gain, bias_values):
    average = jnp.mean(value_rows, axis=(-2, -1), keepdims=True)
    centered = value_rows - average
    variance = jnp.mean(centered * centered, axis=(-2, -1), keepdims=True)
    return centered * lax.rsqrt(variance + vision_epsilon) * gain + bias_values


MESH = pl.DeviceIdType.MESH


def partner(data_index, step, inner, plane):
    if plane is None:
        return lax.rem(data_index + step, inner)
    outer_at, inner_at = data_index // inner, data_index % inner
    if plane:
        return outer_at * inner + lax.rem(inner_at + step, inner)
    count = lax.axis_size("dp") // inner
    return lax.rem(outer_at + step, count) * inner + inner_at


def place(data_index, inner, plane):
    if plane is None:
        return data_index
    return data_index % inner if plane else data_index // inner


def greet(size, inner, plane):
    data_index = lax.axis_index("dp")
    barrier = pltpu.get_barrier_semaphore()
    for step in range(1, size):
        pl.semaphore_signal(
            barrier,
            inc=1,
            device_id={"dp": partner(data_index, step, inner, plane)},
            device_id_type=MESH,
        )
    pl.semaphore_wait(barrier, size - 1)


def exchange_kernel(size, inner, plane, x_ref, o_ref, send_sem, recv_sem, own_sem):
    data_index = lax.axis_index("dp")
    me = place(data_index, inner, plane)
    own = pltpu.make_async_copy(x_ref.at[me], o_ref.at[me], own_sem)
    own.start()
    greet(size, inner, plane)
    copies = []
    for step in range(1, size):
        target = partner(data_index, step, inner, plane)
        copy = pltpu.make_async_remote_copy(
            src_ref=x_ref.at[place(target, inner, plane)],
            dst_ref=o_ref.at[me],
            send_sem=send_sem.at[step - 1],
            recv_sem=recv_sem.at[step - 1],
            device_id={"dp": target},
            device_id_type=MESH,
        )
        copy.start()
        copies.append(copy)
    own.wait()
    for copy in copies:
        copy.wait()


def greet_both(inner):
    data_index = lax.axis_index("dp")
    outer = lax.axis_size("dp") // inner
    barrier = pltpu.get_barrier_semaphore()
    for plane, size in ((True, inner), (False, outer)):
        for step in range(1, size):
            pl.semaphore_signal(
                barrier,
                inc=1,
                device_id={"dp": partner(data_index, step, inner, plane)},
                device_id_type=MESH,
            )
    pl.semaphore_wait(barrier, inner + outer - 2)


def reduce_kernel(
    inner, chunks, rows, x_ref, o_ref, held, mid, got, send_1, recv_1, send_2, recv_2
):
    data_index = lax.axis_index("dp")
    outer, tokens, columns = mid.shape
    wide = columns // chunks
    me, me_outer = place(data_index, inner, True), place(data_index, inner, False)
    greet_both(inner)
    first, second = {}, {}
    for chunk in range(chunks):
        part = pl.ds(chunk * wide, wide)
        for step in range(1, inner):
            target = partner(data_index, step, inner, True)
            first[chunk, step] = pltpu.make_async_remote_copy(
                src_ref=x_ref.at[:, place(target, inner, True), :, part],
                dst_ref=held.at[step - 1, :, :, part],
                send_sem=send_1.at[step - 1, chunk],
                recv_sem=recv_1.at[step - 1, chunk],
                device_id={"dp": target},
                device_id_type=MESH,
            )
            first[chunk, step].start()
    for chunk in range(chunks):
        part = pl.ds(chunk * wide, wide)
        for step in range(1, inner):
            first[chunk, step].wait_recv()

        def add(at, carry):
            row = lax.rem(me_outer + 1 + at // (tokens // rows), outer)
            window = pl.ds(pl.multiple_of(at % (tokens // rows) * rows, rows), rows)
            total = x_ref[row, me, window, part].astype(jnp.float32)
            for step in range(1, inner):
                total = total + held[step - 1, row, window, part].astype(jnp.float32)
            mid[row, window, part] = total.astype(mid.dtype)
            return carry

        lax.fori_loop(0, outer * (tokens // rows), add, 0)
        for step in range(1, outer):
            target = partner(data_index, step, inner, False)
            second[chunk, step] = pltpu.make_async_remote_copy(
                src_ref=mid.at[place(target, inner, False), :, part],
                dst_ref=got.at[step - 1, :, part],
                send_sem=send_2.at[step - 1, chunk],
                recv_sem=recv_2.at[step - 1, chunk],
                device_id={"dp": target},
                device_id_type=MESH,
            )
            second[chunk, step].start()
    for chunk in range(chunks):
        part = pl.ds(chunk * wide, wide)
        for step in range(1, outer):
            second[chunk, step].wait_recv()

        def finish(at, carry):
            window = pl.ds(pl.multiple_of(at * rows, rows), rows)
            total = mid[me_outer, window, part].astype(jnp.float32)
            for step in range(1, outer):
                total = total + got[step - 1, window, part].astype(jnp.float32)
            o_ref[window, part] = total.astype(o_ref.dtype)
            return carry

        lax.fori_loop(0, tokens // rows, finish, 0)
    for copy in list(first.values()) + list(second.values()):
        copy.wait_send()


def reduce_blocks(partial, number):
    outer, inner, tokens, columns = partial.shape
    chunks = 4
    return pl.pallas_call(
        functools.partial(reduce_kernel, inner, chunks, math.gcd(tokens, 16)),
        out_shape=jax.ShapeDtypeStruct((tokens, columns), partial.dtype),
        in_specs=[pl.BlockSpec(memory_space=pltpu.VMEM)],
        out_specs=pl.BlockSpec(memory_space=pltpu.VMEM),
        scratch_shapes=[
            pltpu.VMEM((inner - 1, outer, tokens, columns), partial.dtype),
            pltpu.VMEM((outer, tokens, columns), partial.dtype),
            pltpu.VMEM((outer - 1, tokens, columns), partial.dtype),
            pltpu.SemaphoreType.DMA((inner - 1, chunks)),
            pltpu.SemaphoreType.DMA((inner - 1, chunks)),
            pltpu.SemaphoreType.DMA((outer - 1, chunks)),
            pltpu.SemaphoreType.DMA((outer - 1, chunks)),
        ],
        compiler_params=pltpu.CompilerParams(
            collective_id=number, has_side_effects=True, vmem_limit_bytes=40 << 20
        ),
        cost_estimate=pl.CostEstimate(
            flops=0, bytes_accessed=60 * partial.size, transcendentals=0
        ),
    )(partial)


def product_kernel(inner, count, tile, rows, *refs):
    a_refs = refs[:count]
    w_ref, o_ref, leaving, held, send_sem, recv_sem = refs[count:]
    depth = w_ref.shape[0] // count
    tensor_index = lax.axis_index("tensor")
    data_index = lax.axis_index("dp")
    tiles = o_ref.shape[1] // tile

    def compute(block, dst_ref, low, high):
        def one(at, carry):
            part = pl.ds(pl.multiple_of(at * tile, tile), tile)
            total = None
            for ahead, a_ref in enumerate(a_refs):
                start = lax.rem(tensor_index + count - ahead, count) * depth
                rows_at = pl.ds(pl.multiple_of(start, depth), depth)
                term = jnp.dot(
                    a_ref[block], w_ref[rows_at, part], preferred_element_type=jnp.float32
                )
                total = term if total is None else total + term
            dst_ref[:, part] = total.astype(dst_ref.dtype)
            return carry

        lax.fori_loop(low, high, one, 0)

    greet(inner, inner, True)
    copies = []
    for step in range(1, inner + 1):
        target = partner(data_index, step, inner, True)
        block = place(target, inner, True)
        dst_ref = leaving.at[step - 1] if step < inner else o_ref
        compute(block, dst_ref, 0, 1)
        if copies:
            copies[-1].start()
        compute(block, dst_ref, 1, tiles)
        if step < inner:
            copies.append(
                pltpu.make_async_remote_copy(
                    src_ref=leaving.at[step - 1],
                    dst_ref=held.at[step - 1],
                    send_sem=send_sem.at[step - 1],
                    recv_sem=recv_sem.at[step - 1],
                    device_id={"dp": target},
                    device_id_type=MESH,
                )
            )
    for copy in copies:
        copy.wait_recv()

    def add(at, carry):
        window = pl.ds(pl.multiple_of(at * rows, rows), rows)
        total = o_ref[window, :]
        for step in range(1, inner):
            total = total + held[step - 1, window, :].astype(jnp.float32)
        o_ref[window, :] = total
        return carry

    lax.fori_loop(0, o_ref.shape[0] // rows, add, 0)
    for copy in copies:
        copy.wait_send()


def product_blocks(pieces, weight, number):
    inner, rows, depth = pieces[0].shape
    columns = weight.shape[1]
    count = len(pieces)
    return pl.pallas_call(
        functools.partial(
            product_kernel, inner, count, math.gcd(columns, 512), math.gcd(rows, 16)
        ),
        out_shape=jax.ShapeDtypeStruct((rows, columns), jnp.float32),
        in_specs=[pl.BlockSpec(memory_space=pltpu.VMEM)] * (count + 1),
        out_specs=pl.BlockSpec(memory_space=pltpu.VMEM),
        scratch_shapes=[
            pltpu.VMEM((inner - 1, rows, columns), jnp.bfloat16),
            pltpu.VMEM((inner - 1, rows, columns), jnp.bfloat16),
            pltpu.SemaphoreType.DMA((inner - 1,)),
            pltpu.SemaphoreType.DMA((inner - 1,)),
        ],
        compiler_params=pltpu.CompilerParams(
            collective_id=number, has_side_effects=True, vmem_limit_bytes=56 << 20
        ),
        cost_estimate=pl.CostEstimate(
            flops=2 * count * inner * rows * depth * columns,
            bytes_accessed=200 << 20,
            transcendentals=0,
        ),
    )(*pieces, weight)


def exchange(blocks, inner, plane, number):
    size = blocks.shape[0]
    return pl.pallas_call(
        functools.partial(exchange_kernel, size, inner, plane),
        out_shape=jax.ShapeDtypeStruct(blocks.shape, blocks.dtype),
        in_specs=[pl.BlockSpec(memory_space=pltpu.VMEM)],
        out_specs=pl.BlockSpec(memory_space=pltpu.VMEM),
        scratch_shapes=[
            pltpu.SemaphoreType.DMA((size - 1,)),
            pltpu.SemaphoreType.DMA((size - 1,)),
            pltpu.SemaphoreType.DMA,
        ],
        compiler_params=pltpu.CompilerParams(
            collective_id=number, has_side_effects=True, vmem_limit_bytes=40 << 20
        ),
        cost_estimate=pl.CostEstimate(
            flops=0, bytes_accessed=40 * blocks.size, transcendentals=0
        ),
    )(blocks)


def tensor_pieces(block):
    count = lax.axis_size("tensor")
    pieces = [block]
    for step in range(1, count):
        ring = [(at, (at + step) % count) for at in range(count)]
        pieces.append(lax.ppermute(block, "tensor", ring))
    return pieces


def attend_kernel(group, q_ref, k_ref, v_ref, cos_ref, sin_ref, o_ref):
    cosine, sine = cos_ref[...], sin_ref[...]

    def turn(rows):
        return (rows * cosine + pltpu.roll(rows, HEAD_WIDTH // 2, 1) * sine).astype(jnp.bfloat16)

    key_rows = turn(k_ref[...])
    value_rows = v_ref[...].astype(jnp.bfloat16)
    seq_len = key_rows.shape[0]
    row_at = lax.broadcasted_iota(jnp.int32, (seq_len, seq_len), 0)
    column_at = lax.broadcasted_iota(jnp.int32, (seq_len, seq_len), 1)
    for head in range(group):
        part = pl.ds(head * HEAD_WIDTH, HEAD_WIDTH)
        query_rows = turn(q_ref[:, part])
        scores = lax.dot_general(
            query_rows, key_rows, (((1,), (1,)), ((), ())), preferred_element_type=jnp.float32
        ) * HEAD_WIDTH ** (-0.5)
        scores = jnp.where(row_at >= column_at, scores, -1e30)
        exponentials = jnp.exp(scores - jnp.max(scores, axis=-1, keepdims=True))
        weights = exponentials / jnp.sum(exponentials, axis=-1, keepdims=True)
        context = jnp.dot(
            weights.astype(jnp.bfloat16), value_rows, preferred_element_type=jnp.float32
        )
        o_ref[:, part] = context.astype(o_ref.dtype)


def attend(product, part_query):
    seq_len, columns = product.shape
    group = QUERY_HEADS // KEY_VALUE_HEADS
    local_kv = part_query // HEAD_WIDTH // group
    key_at = part_query // HEAD_WIDTH
    half_width = HEAD_WIDTH // 2
    exponents = jnp.arange(half_width, dtype=jnp.float32) * (2.0 / HEAD_WIDTH)
    frequency = rope_base ** (-exponents)
    angles = jnp.arange(seq_len, dtype=jnp.float32)[:, None] * frequency[None, :]
    cosine, sine = jnp.cos(angles), jnp.sin(angles)
    cosine = jnp.concatenate([cosine, cosine], axis=1)
    sine = jnp.concatenate([-sine, sine], axis=1)
    table = pl.BlockSpec((seq_len, HEAD_WIDTH), lambda g: (0, 0))
    return pl.pallas_call(
        functools.partial(attend_kernel, group),
        grid=(local_kv,),
        out_shape=jax.ShapeDtypeStruct((seq_len, part_query), jnp.bfloat16),
        in_specs=[
            pl.BlockSpec((seq_len, group * HEAD_WIDTH), lambda g: (0, g)),
            pl.BlockSpec((seq_len, HEAD_WIDTH), lambda g: (0, key_at + g)),
            pl.BlockSpec((seq_len, HEAD_WIDTH), lambda g: (0, key_at + local_kv + g)),
            table,
            table,
        ],
        out_specs=pl.BlockSpec((seq_len, group * HEAD_WIDTH), lambda g: (0, g)),
        compiler_params=pltpu.CompilerParams(vmem_limit_bytes=24 << 20),
    )(product, product, product, cosine, sine)


def per_device(
    vis_rows,
    ln_gain,
    ln_bias,
    proj_weight,
    text_rows,
    attn_gain,
    w_query,
    key_value_weight,
    tile_counts,
    image_offsets,
):
    data_count = lax.axis_size("dp")
    data_index = lax.axis_index("dp")
    tensor_count = lax.axis_size("tensor")
    tensor_index = lax.axis_index("tensor")
    tile_rows, tile_tok, merge_count, part_width = vis_rows.shape
    vision_width = ln_gain.shape[1]
    part_model = proj_weight.shape[2]
    token_count = tile_rows * tile_tok
    inner = 1 << (int(math.log2(data_count)) // 2)
    outer = data_count // inner
    columns_of = [[at * inner + b for at in range(outer)] for b in range(inner)]
    depth = w_query.shape[0]
    weight = jnp.concatenate([w_query, key_value_weight.reshape(depth, -1)], axis=1)
    weight = lax.all_gather(weight, "dp", axis=0, tiled=True, axis_index_groups=columns_of)

    max_tiles = 2 * tile_rows
    slot_count = (max_tiles + data_count - 1) // data_count
    tile_ends = jnp.cumsum(tile_counts)
    tile_firsts = tile_ends - tile_counts
    sample_ids = jnp.arange(data_count, dtype=jnp.int32)
    tiles_here = jnp.arange(tile_rows, dtype=jnp.int32) * data_count + data_index
    owners = jnp.sum((tile_ends[None, :] <= tiles_here[:, None]).astype(jnp.int32), axis=1)
    owner_first = jnp.sum(
        jnp.where(sample_ids[None, :] == owners[:, None], tile_firsts[None, :], 0), axis=1
    )
    slots = (tiles_here - owner_first) // data_count
    is_mine = sample_ids == data_index
    my_first = jnp.sum(jnp.where(is_mine, tile_firsts, 0))
    my_count = jnp.sum(jnp.where(is_mine, tile_counts, 0))
    tile_order = jnp.arange(max_tiles, dtype=jnp.int32)
    sources = (my_first + tile_order) % data_count
    slot_index = tile_order // data_count
    image_span = max_tiles * tile_tok

    pieces = tensor_pieces(vis_rows.reshape(token_count, merge_count, part_width))
    whole = jnp.zeros((token_count, merge_count, vision_width), vis_rows.dtype)
    for step, piece in enumerate(pieces):
        start = (tensor_index - step) % tensor_count * part_width
        whole = lax.dynamic_update_slice_in_dim(whole, piece, start, 2)
    normed_vis = layer_norm(whole.astype(jnp.float32), ln_gain, ln_bias).astype(jnp.bfloat16)
    feature = vision_width // data_count
    blocks = normed_vis.reshape(token_count, merge_count, data_count, feature)
    blocks = blocks.transpose(2, 0, 1, 3).reshape(data_count, token_count, merge_count * feature)
    blocks = exchange(blocks, data_count, None, 0)
    proj = proj_weight.transpose(1, 0, 2).reshape(merge_count * feature, part_model)
    partial = jnp.dot(
        blocks.reshape(data_count * token_count, merge_count * feature),
        proj,
        preferred_element_type=jnp.float32,
    ).astype(jnp.bfloat16)
    image_cols = reduce_blocks(
        partial.reshape(outer, inner, token_count, part_model), 1
    ).reshape(tile_rows, tile_tok, part_model)

    empty_slots = jnp.zeros((data_count, slot_count) + image_cols.shape[1:], jnp.bfloat16)
    routed = empty_slots.at[owners, slots].set(image_cols)
    received = exchange(routed, data_count, None, 3)
    arrived = received[sources, slot_index]
    arrived = arrived.reshape(image_span, part_model)
    start_row = image_offsets[0]
    sequence = text_rows[0]
    current = lax.dynamic_slice_in_dim(sequence, start_row, image_span, 0)
    is_image = jnp.repeat(tile_order < my_count, tile_tok)[:, None]
    combined = jnp.where(is_image, arrived, current)
    sequence = lax.dynamic_update_slice_in_dim(sequence, combined, start_row, 0)

    seq_len = sequence.shape[0]
    model_width = attn_gain.shape[0]
    seq_float = sequence.astype(jnp.float32)
    squares = lax.psum(jnp.sum(seq_float * seq_float, axis=-1), "tensor")[:, None]
    gain = lax.dynamic_slice_in_dim(attn_gain, tensor_index * part_model, part_model, 0)
    normalized = (
        seq_float * lax.rsqrt(squares / model_width + decoder_epsilon) * gain
    ).astype(jnp.bfloat16)
    held_rows = part_model // depth // inner
    normalized = normalized.reshape(seq_len, held_rows, inner, depth).transpose(2, 0, 1, 3)
    normalized = exchange(
        normalized.reshape(inner, seq_len, held_rows * depth), inner, True, 4
    )
    pieces = tensor_pieces(normalized)
    product = product_blocks(pieces, weight, 5)
    part_query = w_query.shape[1]
    context = attend(product, part_query)
    return context.reshape(1, seq_len, context.shape[1])


def solution(mesh):
    in_specs = (
        P(None, "dp", None, "tensor"),
        P(),
        P(),
        P("dp", None, "tensor"),
        P("dp", None, "tensor"),
        P(),
        P("dp", "tensor"),
        P("dp", None, "tensor"),
        P(),
        P("dp"),
    )
    out_specs = P("dp", None, "tensor")
    return jax.shard_map(
        per_device, mesh=mesh, in_specs=in_specs, out_specs=out_specs, check_vma=False
    )
```
